256 devices in a mesh: dp: 4 (over x), expert: 64 (over y, z, core).
Axes of the slice: x: 4, y: 4, z: 8, core: 2. Of those that a mesh axis runs over, the one named last changes fastest.
Arguments:
- tokens: bfloat16 [32768, 2048], P(('dp', 'expert')), may hold values from -6 to 6
- routes: int32 [32768, 8], P(('dp', 'expert')), may hold values from 0 to 127, all different within a row
- route_weight: float32 [32768, 8], P(('dp', 'expert')), may hold values from 0.05 to 0.5
- bias: float32 [128], replicated, may hold values from -3 to 3
- w_gate: bfloat16 [128, 768, 2048], P('expert', 'dp'), may hold values from -0.125 to 0.125
- w_up: bfloat16 [128, 768, 2048], P('expert', 'dp'), may hold values from -0.125 to 0.125
- w_down: bfloat16 [128, 768, 2048], P('expert', 'dp'), may hold values from -0.21875 to 0.21875
Outputs:
- mixed: bfloat16 [32768, 2048], P(('dp', 'expert'))
- new_bias: float32 [128], replicated
- counts: int32 [128], replicated
The draws below stay inside these ranges and needn't reach their ends.
Inputs may be any that keep to these rules, and one draw needn't show every extreme that they name: `routes`: each token names 8 different experts.
All inputs are finite; a program needn't handle non-finite values.
Results may differ from the reference program's by a relative error of at most 0.0057.
Values may be sent and summed in bfloat16 or wider, within the bound.
No kernel may reach another device: no remote copies, remote signals or barrier semaphores. Data moves between devices by JAX's collectives and lax.ppermute only.
A program may use at most 128 MiB of HBM per device.

```python
import jax
import jax.numpy as jnp
from jax import lax

D = 2048
FF = 768
TOP = 8
TOK_DEV = 128
EXPERTS = 128
TOKENS = 32768
CAP = 10


def level_of(rng, extent, shards, smallest, top_value):
    loudness, own = 1.0, jax.random.fold_in(rng, 6)
    for position, shards_of in shards:
        heights = jnp.exp(jax.random.uniform(jax.random.fold_in(own, position), (shards_of,), jnp.float32, smallest / len(shards), top_value / len(shards)))
        loudness = loudness * jnp.repeat(heights, extent[position] // shards_of).reshape([-1 if axis == position else 1 for axis in range(len(extent))])
    return loudness


def different_ones(key, rows, amount, top, lift):
    order = jax.random.permutation(jax.random.fold_in(key, 1), amount)
    favour = order
    for power in range(3):
        favour = favour * favour // amount
    favour = favour * lift // amount
    lots = jax.random.randint(jax.random.fold_in(key, 2), (rows, amount), 0, 4096) + favour
    holders = jax.random.permutation(jax.random.fold_in(key, 3), rows)[jnp.arange(amount) % rows]
    lots = jnp.where(jnp.arange(rows)[:, None] == holders[None, :], 1 << 14, lots)
    merit = lots * amount + jnp.arange(amount)
    return lax.top_k(merit.astype(jnp.int32), top)[1].astype(jnp.int32)


def scatter_about(own_key, extent, width, reach, shards=(), held_as=jnp.bfloat16):
    drawn = jax.random.normal(own_key, extent, jnp.float32) * width
    if len(shards) > 0:
        drawn = level_of(own_key, extent, shards, -0.22, 0.18) * drawn
    return jnp.clip(drawn, min=-reach, max=reach).astype(held_as)


def setup_inputs(seed: int = 0) -> dict:
    key_of = jax.random.split(jax.random.key(seed), 8)
    tokens = scatter_about(key_of[0], (TOKENS, D), 1.0, 6.0, ((0, 256),))
    routes = different_ones(key_of[1], TOKENS, EXPERTS, TOP, 512)
    route_weight = jnp.clip(0.05 + 0.45 * jax.random.uniform(key_of[2], (TOKENS, TOP), jnp.float32) ** level_of(key_of[2], (TOKENS, TOP), ((0, 256),), -0.2, 0.2), 0.05, 0.5)
    bias = scatter_about(key_of[3], (EXPERTS,), 0.5, 3.0, (), jnp.float32)
    w_gate = scatter_about(key_of[4], (EXPERTS, FF, D), D ** -0.5, 0.125, ((0, 64), (1, 4)))
    w_up = scatter_about(key_of[5], (EXPERTS, FF, D), D ** -0.5, 0.125, ((0, 64), (1, 4)))
    w_down = scatter_about(key_of[6], (EXPERTS, FF, D), FF ** -0.5, 0.21875, ((0, 64), (1, 4)))
    return dict(tokens=tokens, routes=routes, route_weight=route_weight, bias=bias, w_gate=w_gate, w_up=w_up, w_down=w_down)


bias_rate = 0.05


def reference(tokens, routes, route_weight, bias, w_gate, w_up, w_down):
    sources = TOKENS // TOK_DEV
    entries = TOK_DEV * TOP
    block_routes = routes.reshape(sources, entries)
    labels = jnp.arange(EXPERTS, dtype=jnp.int32)

    def rank_block(block_row):
        picked = (block_row[:, None] == labels[None, :]).astype(jnp.int32)
        running = jnp.cumsum(picked, axis=0) - picked
        return jnp.sum(running * picked, axis=1).astype(jnp.int32), jnp.sum(picked, axis=0).astype(jnp.int32)

    slot_rank, block_counts = lax.map(rank_block, block_routes)
    counts = jnp.sum(block_counts, axis=0).astype(jnp.int32)
    kept_mask = slot_rank < CAP
    source_index = jnp.arange(sources, dtype=jnp.int32)[:, None]
    token_index = (source_index * TOK_DEV + jnp.arange(entries, dtype=jnp.int32)[None, :] // TOP).astype(jnp.int32)
    slot_total = EXPERTS * sources * CAP
    slot_index = jnp.where(kept_mask, block_routes * (sources * CAP) + source_index * CAP + slot_rank, slot_total).astype(jnp.int32)
    token_table = jnp.zeros((slot_total + 1,), jnp.int32).at[slot_index.reshape(-1)].set(token_index.reshape(-1))
    token_table = token_table[:slot_total].reshape(EXPERTS, sources * CAP)
    entry_weight = jnp.where(kept_mask, route_weight.reshape(sources, entries), jnp.float32(0.0)).astype(jnp.float32)
    weight_table = jnp.zeros((slot_total + 1,), jnp.float32).at[slot_index.reshape(-1)].set(entry_weight.reshape(-1))
    weight_table = weight_table[:slot_total].reshape(EXPERTS, sources * CAP)

    def one_expert(carry_sum, expert_items):
        slot_tokens, slot_weights, gate_w, up_w, down_w = expert_items
        picked_rows = tokens[slot_tokens]
        gate_act = lax.dot_general(picked_rows, gate_w, (((1,), (1,)), ((), ())), preferred_element_type=jnp.float32)
        up_act = lax.dot_general(picked_rows, up_w, (((1,), (1,)), ((), ())), preferred_element_type=jnp.float32)
        hidden = (jax.nn.silu(gate_act) * up_act).astype(jnp.bfloat16)
        expert_out = jnp.dot(hidden, down_w, preferred_element_type=jnp.float32).astype(jnp.bfloat16)
        return carry_sum.at[slot_tokens].add(expert_out.astype(jnp.float32) * slot_weights[:, None]), None

    summed, _ = lax.scan(one_expert, jnp.zeros((TOKENS, D), jnp.float32), (token_table, weight_table, w_gate, w_up, w_down))
    mixed = summed.astype(jnp.bfloat16)
    new_bias = bias + bias_rate * jnp.sign((TOKENS * TOP - EXPERTS * counts).astype(jnp.float32))
    return mixed, new_bias, counts
```

```python
import functools

import jax
import jax.numpy as jnp
from jax import lax
from jax.experimental import pallas as pl
from jax.experimental.pallas import tpu as pltpu
from jax.sharding import Mesh
from jax.sharding import PartitionSpec as P


YZC = ("expert_0", "expert_1", "expert_2")
ALL = ("dp", "expert_0", "expert_1", "expert_2")
YC = ("expert_0", "expert_2")
CAP = 10
BLOCKS = 8
PEERS = 8
ROWS = CAP * BLOCKS
BF = jnp.bfloat16
F32 = jnp.float32
bias_rate = 0.05
VMEM = pl.BlockSpec(memory_space=pltpu.VMEM)
SMEM = pl.BlockSpec(memory_space=pltpu.SMEM)


def call(kernel, outs, args, specs, scratch, flops, name):
    return pl.pallas_call(
        kernel,
        out_shape=outs,
        in_specs=specs,
        out_specs=jax.tree.map(lambda _: VMEM, outs),
        scratch_shapes=scratch,
        name=name,
        cost_estimate=pl.CostEstimate(flops=flops, bytes_accessed=1 << 20, transcendentals=0),
        compiler_params=pltpu.CompilerParams(vmem_limit_bytes=40 << 20),
    )(*args)


def select_kernel(pos, rw, *refs):
    pieces, outs = refs[:9], refs[9:25]
    key_ref, w_ref, table, hot = refs[25:29]
    y, z, c = pos[0], pos[1], pos[2]
    for p in range(7):
        table[p * 128 : (p + 1) * 128, :] = pieces[p][...]
    table[896:960, :] = pieces[7][...]
    table[960:1024, :] = pieces[8][...]
    i = lax.broadcasted_iota(jnp.int32, (16, 128), 0)
    dy, dc, j = lax.shift_right_logical(i & 7, 1), i & 1, lax.shift_right_logical(i, 3)
    expert = ((y + dy) & 3) * 32 + z * 4 + (c + dc - 2 * c * dc) * 2 + j
    expert = expert.astype(F32)
    picks, weights = [], []
    for p in range(8):
        block = rw[(z + (p + 5)) & 7]
        hit_sum = jnp.zeros((16, 128), F32)
        w_sum = jnp.zeros((16, 128), F32)
        for k in range(8):
            hit = expert == block[k : k + 1, :]
            hit_sum = hit_sum + jnp.where(hit, 1.0, 0.0)
            w_sum = w_sum + jnp.where(hit, block[8 + k : 9 + k, :], 0.0)
        picks.append(hit_sum)
        weights.append(w_sum)
    picked = jnp.concatenate(picks, axis=0)
    before = lax.broadcasted_iota(jnp.int32, (128, 128), 0) < lax.broadcasted_iota(
        jnp.int32, (128, 128), 1
    )
    rank = jnp.dot(picked.astype(BF), jnp.where(before, 1.0, 0.0).astype(BF), preferred_element_type=F32)
    for p in range(8):
        r = rank[p * 16 : (p + 1) * 16, :]
        kept = (picks[p] > 0.5) & (r < CAP - 0.5)
        key_ref[:, p * 128 : (p + 1) * 128] = jnp.where(kept, r + p * CAP, -1.0)
        w_ref[:, p * 128 : (p + 1) * 128] = weights[p]
    row = lax.broadcasted_iota(jnp.int32, (ROWS, 1024), 0).astype(F32)
    for j in range(2):
        for q in range(8):
            n = j * 8 + q
            hot[n * ROWS : (n + 1) * ROWS, :] = jnp.where(row == key_ref[n : n + 1, :], 1.0, 0.0).astype(BF)

    @pl.loop(0, 8)
    def _(n):
        cols = pl.ds(pl.multiple_of(n * 256, 256), 256)
        got = jnp.dot(hot[...], table[:, cols], preferred_element_type=F32).astype(BF)
        for i in range(16):
            outs[i][:, cols] = got[i * ROWS : (i + 1) * ROWS, :]


def spread_kernel(key_ref, w_ref, *refs):
    outs, hot = refs[:2], refs[2]
    row = lax.broadcasted_iota(jnp.int32, (ROWS, 1024), 0).astype(F32)
    for j in range(2):
        for q in range(8):
            n = j * 8 + q
            hot[q * ROWS : (q + 1) * ROWS, :] = jnp.where(
                row == key_ref[n : n + 1, :], w_ref[n : n + 1, :], 0.0
            )
        outs[j][...] = hot[...].T.astype(BF)


def ffn_kernel(halves, *refs):
    x, w = refs[:8], refs[8:13]
    outs = refs[13 : 13 + 8 * halves]
    rows, gate, up, down, hidden = refs[13 + 8 * halves :]
    for i in range(8):
        rows[i * ROWS : (i + 1) * ROWS, :] = x[i][...]
    for i in range(3):
        gate[i * 192 : (i + 1) * 192, :] = w[i][0:192, :]
        up[i * 192 : (i + 1) * 192, :] = w[i][192:384, :]
        down[i * 192 : (i + 1) * 192, :] = w[i][384:576, :]
    gate[576:768, :] = w[3][0:192, :]
    up[576:672, :] = w[3][192:288, :]
    up[672:768, :] = w[4][0:96, :]
    down[576:768, :] = w[4][96:288, :]
    nt = (((1,), (1,)), ((), ()))

    @pl.loop(0, 3)
    def _(n):
        part = pl.ds(pl.multiple_of(n * 256, 256), 256)
        g = lax.dot_general(rows[...], gate[part, :], nt, preferred_element_type=F32)
        u = lax.dot_general(rows[...], up[part, :], nt, preferred_element_type=F32)
        hidden[:, part] = (g / (1.0 + jnp.exp(-g)) * u).astype(BF)

    width = 2048 // halves
    for h in range(halves):

        @pl.loop(0, width // 256)
        def _(n):
            src = pl.ds(pl.multiple_of(h * width + n * 256, 256), 256)
            dst = pl.ds(pl.multiple_of(n * 256, 256), 256)
            got = jnp.dot(hidden[...], down[:, src], preferred_element_type=F32).astype(BF)
            for i in range(8):
                outs[h * 8 + i][:, dst] = got[i * ROWS : (i + 1) * ROWS, :]


def mix_kernel(h, *refs):
    p0, p1 = refs[0], refs[1]
    r0, r1 = refs[2:10], refs[10:18]
    out, rows = refs[18], refs[19]
    for i in range(8):
        rows[i * ROWS : (i + 1) * ROWS, :] = r0[i][:, h * 1024 : (h + 1) * 1024]
        rows[640 + i * ROWS : 640 + (i + 1) * ROWS, :] = r1[i][...]

    @pl.loop(0, 4)
    def _(n):
        cols = pl.ds(pl.multiple_of(n * 256, 256), 256)
        got = jnp.dot(p0[...], rows[0:640, cols], preferred_element_type=F32)
        got += jnp.dot(p1[...], rows[640:1280, cols], preferred_element_type=F32)
        for i in range(8):
            out[i, :, cols] = got[i * 128 : (i + 1) * 128, :]


def shift(array, axis, size, by):
    return lax.ppermute(array, axis, [(i, (i + by) % size) for i in range(size)])


def swap(array, dy, dc):
    pairs = [(y * 2 + c, ((y + dy) % 4) * 2 + (c ^ dc)) for y in range(4) for c in range(2)]
    return lax.ppermute(array, YC, pairs)


def exchange(parts):
    return [parts[0]] + [swap(parts[i], i // 2, i % 2) for i in range(1, 8)]


def give_back(parts):
    return [parts[0]] + [swap(parts[i], -(i // 2), i % 2) for i in range(1, 8)]


def weights_of(own):
    left = shift(own, "dp", 4, 1)
    right = shift(own, "dp", 4, -1)
    half = own.shape[0] // 2
    far_a = shift(left[:half], "dp", 4, 1)
    far_b = shift(right[half:], "dp", 4, -1)
    return [own, left, right, far_a, far_b]


def ring_sum(parts, steps_up, steps_down):
    def chain(steps, sign):
        moving = parts[3 + sign * steps].astype(BF) if steps < 4 else parts[7].astype(BF)
        for s in range(steps - 1, -1, -1):
            moving = shift(moving, "expert_1", 8, sign)
            if s > 0:
                moving = (moving.astype(F32) + parts[3 + sign * s]).astype(BF)
        return moving

    up = chain(steps_up, 1)
    down = chain(steps_down, -1)
    return (parts[3] + up.astype(F32) + down.astype(F32)).astype(BF)


def body(tokens, routes, route_weight, bias, w_gate, w_up, w_down):
    packed = [
        jnp.concatenate([w_gate[e], w_up[e], w_down[e]], axis=0) for e in range(2)
    ]
    rw = jnp.concatenate([routes.T.astype(F32), route_weight.T], axis=0)
    rw_all = lax.all_gather(rw, "expert_1", axis=0, tiled=False)
    ring = {0: tokens}
    for s in range(1, 4):
        ring[-s] = shift(ring[1 - s], "expert_1", 8, 1)
        ring[s] = shift(ring[s - 1], "expert_1", 8, -1)
    far_a = shift(ring[-3][:64], "expert_1", 8, 1)
    far_b = shift(ring[3][64:], "expert_1", 8, -1)
    pos = jnp.stack(
        [lax.axis_index("expert_0"), lax.axis_index("expert_1"), lax.axis_index("expert_2")]
    ).astype(jnp.int32)
    shape = jax.ShapeDtypeStruct
    picked = call(
        select_kernel,
        [shape((ROWS, 2048), BF)] * 16 + [shape((16, 1024), F32)] * 2,
        [pos, rw_all] + [ring[d] for d in range(-3, 4)] + [far_a, far_b],
        [SMEM] + [VMEM] * 10,
        [pltpu.VMEM((1024, 2048), BF), pltpu.VMEM((1280, 1024), BF)],
        5 << 30,
        "select",
    )
    sent0, sent1, key, weight = picked[:8], picked[8:16], picked[16], picked[17]
    x0 = exchange(sent0)
    x1 = exchange(sent1)
    spread = call(
        spread_kernel,
        [shape((1024, 640), BF)] * 2,
        [key, weight],
        [VMEM] * 2,
        [pltpu.VMEM((640, 1024), F32)],
        4 << 30,
        "spread",
    )

    def ffn(x, w, halves):
        return call(
            functools.partial(ffn_kernel, halves),
            [shape((ROWS, 2048 // halves), BF)] * (8 * halves),
            x + w,
            [VMEM] * 13,
            [pltpu.VMEM((640, 2048), BF)]
            + [pltpu.VMEM((768, 2048), BF)] * 3
            + [pltpu.VMEM((640, 768), BF)],
            6 << 30,
            "ffn",
        )

    w0 = weights_of(packed[0])
    w1 = weights_of(packed[1])
    r0 = give_back(ffn(x0, w0, 1))
    y1 = ffn(x1, w1, 2)
    r1 = [give_back(y1[:8]), give_back(y1[8:])]
    mixed = []
    for h in range(2):
        parts = call(
            functools.partial(mix_kernel, h),
            shape((8, 128, 1024), F32),
            list(spread) + list(r0) + list(r1[h]),
            [VMEM] * 18,
            [pltpu.VMEM((1280, 1024), BF)],
            3 << 30,
            "mix",
        )
        up, down = (4, 3) if h == 0 else (3, 4)
        mixed.append(ring_sum(parts, up, down))
    mixed = jnp.concatenate(mixed, axis=1)

    experts = bias.shape[0]
    labels = jnp.arange(experts, dtype=jnp.int32)
    local = jnp.sum((routes.T[:, None, :] == labels[None, :, None]).astype(F32), axis=(0, 2))
    totals = lax.psum(local, ALL)
    mean_load = 32768 * 8
    new_bias = bias + bias_rate * jnp.sign(mean_load - experts * totals)
    return (mixed, new_bias, totals.astype(jnp.int32))


def solution(mesh):
    torus = Mesh(mesh.devices.reshape(4, 4, 8, 2), ALL)
    placed = (
        P(ALL, None),
        P(ALL, None),
        P(ALL, None),
        P(),
        P(YZC, "dp", None),
        P(YZC, "dp", None),
        P(YZC, "dp", None),
    )
    return jax.shard_map(
        body, mesh=torus, in_specs=placed, out_specs=(P(ALL, None), P(), P()), check_vma=False
    )
```
